32 devices in a mesh: rows: 8 (over z, y), grp: 4 (over x, core).
Axes of the slice: x: 2, y: 2, z: 4, core: 2. Of those that a mesh axis runs over, the one named last changes fastest.
Arguments:
- owner: int32 [1024, 24, 3], P('rows', 'grp'), may hold values from 0 to 7, as said below
- offset: int32 [1024, 24, 3], P('rows', 'grp'), may hold values from 0 to 511
- tables: float32 [12, 4096, 128], P('grp', 'rows'), may hold values from -6 to 6
- w_first: bfloat16 [3072, 1024], P('grp'), may hold values from -0.109375 to 0.109375
- b_first: float32 [1024], replicated, may hold values from -3 to 3
- w_out: float32 [1024], replicated, may hold values from -0.1875 to 0.1875
- labels: int32 [1024], P('rows'), may hold values 0 or 1
Outputs:
- table_grad: float32 [12, 4096, 128], P('grp', 'rows')
- losses: float32 [1024], P(('rows', 'grp'))
The draws below stay inside these ranges and needn't reach their ends.
Inputs may be any that keep to these rules, and one draw needn't show every extreme that they name: Of the lookups of one device (its 128 samples and 6 features, all three hashes) at most 1032 name one owner, and in every draw some owner gets exactly 1032. Among the lookups of one device to one owner for one table, at most 114 distinct offsets occur, and that bound is reached in every draw.
All inputs are finite; a program needn't handle non-finite values. No bound on the sum of `labels` on one device may be relied on, other than what follows from the above.
Results may differ from the reference program's by a relative error of at most 0.005.
Values may be sent and summed in bfloat16 or wider, within the bound.
A program may use at most 64 MiB of HBM per device.

```python
import jax
import jax.numpy as jnp
from jax import lax

E = 128
H = 1024
F_GRP = 6
B_DEV = 128
ROWS_DEV = 512
BATCH = 1024
FEATURES = 24
TAB_ROWS = 4096
HOTK = 344
UNIQ = 114
N_GRP = 4


def layout_pair(key):
    row_devices = BATCH // B_DEV
    group_devices = FEATURES // F_GRP
    block_size = B_DEV * F_GRP
    base_key = jax.random.fold_in(key, 7001)

    def device_block(block_key):
        subkeys = jax.random.split(block_key, 4)
        hot_owner = jax.random.randint(subkeys[0], (), 0, row_devices)
        rank_of = jnp.stack([jax.random.permutation(jax.random.fold_in(subkeys[1], column), block_size) for column in range(3)], axis=1).astype(jnp.int32)
        spread_owner = (hot_owner + 1 + (rank_of - HOTK) % (row_devices - 1)) % row_devices
        owners = jnp.where(rank_of < HOTK, hot_owner, spread_owner).astype(jnp.int32)
        pool_pick = jnp.where(rank_of < HOTK, rank_of % UNIQ, jax.random.randint(subkeys[2], (block_size, 3), 0, UNIQ))
        pool_base = jax.random.randint(subkeys[3], (row_devices, 3), 0, ROWS_DEV)
        pool_step = ROWS_DEV // UNIQ
        chosen_base = pool_base[owners, jnp.arange(3, dtype=jnp.int32)[None, :]]
        offsets = (chosen_base + pool_pick * pool_step) % ROWS_DEV
        return (owners.reshape(B_DEV, F_GRP, 3), offsets.astype(jnp.int32).reshape(B_DEV, F_GRP, 3))
    block_keys = jax.random.split(base_key, row_devices * group_devices)
    owners, offsets = jax.vmap(device_block)(block_keys)
    owners = owners.reshape(row_devices, group_devices, B_DEV, F_GRP, 3).transpose(0, 2, 1, 3, 4).reshape(BATCH, FEATURES, 3)
    offsets = offsets.reshape(row_devices, group_devices, B_DEV, F_GRP, 3).transpose(0, 2, 1, 3, 4).reshape(BATCH, FEATURES, 3)
    return (owners, offsets)


def draw_owner(key, part):
    return layout_pair(key)[0]


def draw_offset(key, part):
    return layout_pair(key)[1]


def place_ends(result, stream_key, least, top_value):
    longest = result.shape.index(max(result.shape))
    spots = []
    for shift in (0, 1):
        where = [jax.random.randint(jax.random.fold_in(stream_key, axis), (), 0, length) for axis, length in enumerate(result.shape)]
        where[longest] = (where[longest] + shift) % result.shape[longest]
        spots.append(tuple(where))
    return result.at[spots[0]].set(least).at[spots[1]].set(top_value)


def levels(rng, dims, cuts, low, largest):
    def one(dim, parts):
        draws = jax.random.uniform(jax.random.fold_in(jax.random.fold_in(rng, 6), dim), (parts,), jnp.float32, low / len(cuts), largest / len(cuts))
        return jnp.repeat(jnp.exp(draws), dims[dim] // parts).reshape((-1,) + (1,) * (len(dims) - dim - 1))

    level = one(*cuts[0])
    for cut in cuts[1:]:
        level = level * one(*cut)
    return level


def normal_values(key, shape, scale, limit, cuts=(), kind=jnp.bfloat16):
    values = jax.random.normal(key, shape, jnp.float32) * scale
    if len(cuts) > 0:
        values = levels(key, shape, cuts, -0.22, 0.18) * values
    return jnp.clip(values, min=-limit, max=limit).astype(kind)


def setup_inputs(seed: int = 0) -> dict:
    key_of = jax.random.split(jax.random.key(seed), 8)
    return {
        "owner": draw_owner(jax.random.fold_in(key_of[7], 71), 0),
        "offset": draw_offset(jax.random.fold_in(key_of[7], 71), 0),
        "tables": normal_values(key_of[2], (3 * N_GRP, TAB_ROWS, E), 1.0, 6.0, ((0, 4), (1, 8)), jnp.float32),
        "w_first": normal_values(key_of[3], (FEATURES * E, H), (FEATURES * E) ** -0.5, 0.109375, ((0, 4),)),
        "b_first": normal_values(key_of[4], (H,), 0.5, 3.0, (), jnp.float32),
        "w_out": normal_values(key_of[5], (H,), H ** -0.5, 0.1875, (), jnp.float32),
        "labels": place_ends((jax.random.randint(key_of[6], (BATCH,), 0, 2) < 1).astype(jnp.int32), jax.random.fold_in(key_of[6], 1), 0, 1),
    }


def reference(owner, offset, tables, w_first, b_first, w_out, labels):
    table_kind = jnp.arange(3, dtype=jnp.int32)
    feature_group = jnp.arange(FEATURES, dtype=jnp.int32) // F_GRP
    table_id = jnp.broadcast_to(feature_group[None, :, None] * 3 + table_kind[None, None, :], owner.shape).astype(jnp.int32)
    row_id = (owner * ROWS_DEV + offset).astype(jnp.int32)
    looked_low = tables[table_id, row_id].astype(jnp.bfloat16)
    looked = lax.optimization_barrier(looked_low).astype(jnp.float32)
    embedded = looked[:, :, 0] * looked[:, :, 1] + looked[:, :, 2]
    features = embedded.reshape(BATCH, FEATURES * E).astype(jnp.bfloat16)
    pre_act = jnp.dot(features, w_first, preferred_element_type=jnp.float32) + b_first
    gate_sig = jax.nn.sigmoid(pre_act)
    logits = jnp.sum(pre_act * gate_sig * w_out, axis=1)
    targets = labels.astype(jnp.float32)
    losses = jax.nn.softplus(logits) - targets * logits
    grad_logit = jax.nn.sigmoid(logits) - targets
    grad_pre = (grad_logit[:, None] * w_out * (gate_sig * (1.0 + pre_act * (1.0 - gate_sig)))).astype(jnp.bfloat16)
    grad_emb = jnp.dot(grad_pre, w_first.T, preferred_element_type=jnp.float32).reshape(BATCH, FEATURES, E)
    row_grads = jnp.stack([grad_emb * looked[:, :, 1], grad_emb * looked[:, :, 0], grad_emb], axis=2)
    table_grad = jnp.zeros((3 * N_GRP, TAB_ROWS, E), jnp.float32).at[table_id, row_id].add(row_grads)
    return table_grad, losses
```

```python
import functools

import jax
import jax.numpy as jnp
from jax import lax
from jax.experimental import pallas as pl
from jax.experimental.pallas import tpu as pltpu
from jax.sharding import PartitionSpec as P

BF16 = jnp.bfloat16
F32 = jnp.float32
CHUNKS = 4
ORDER = (0, 1, 3, 2)
MIB = 1024 * 1024


def iota(shape, dim):
    return lax.broadcasted_iota(jnp.int32, shape, dim)


def ones_where(mask):
    return jnp.where(mask, 1.0, 0.0).astype(BF16)


def join_bands(bands, starts, width, total):
    cuts = sorted({0, total, *starts, *(min(s + width, total) for s in starts)})
    pieces = []
    for lo, hi in zip(cuts[:-1], cuts[1:]):
        piece = None
        for band, s in zip(bands, starts):
            if s <= lo and hi <= s + width:
                part = band[lo - s : hi - s]
                piece = part if piece is None else piece + part
        pieces.append(piece)
    return jnp.concatenate(pieces, axis=0).astype(BF16)


def mm(a, b):
    return jnp.dot(a, b, preferred_element_type=F32)


def kernel(
    R, G, cap, fgrp, starts, width,
    own_ref, off_ref, lab_ref, tab_hbm, w_hbm, b_ref, wo_ref,
    tg_ref, loss_ref,
    idx_ref, tab, tb, w, col, of, ranked_bf, req_send, req_recv, fet_send, rows, looked,
    p_ref, pt_ref, st_ref, part_f32, part_send, swap_recv, pair_send, pair_recv, gp, rg, g_send, g_recv,
    local_sem, ss0, rs0, ss1, rs1, ss2, rs2, ssp, rsp, ssg, rsg,
):
    me = lax.axis_index("rows")
    mg = lax.axis_index("grp")
    n_rows = tab.shape[1]
    emb = tab.shape[2]
    nl = idx_ref.shape[1]
    per = nl // 3
    bdev = per // fgrp
    share = bdev // G
    r8 = R * 8
    slots = R * width
    fan = R // CHUNKS
    chunk = fan * width
    my_chunk = lax.div(me, fan)
    side_of = lax.rem(me, fan)
    sent = -(-cap // 8) * 8

    total = fet_send.shape[1]
    joined = functools.partial(join_bands, starts=starts, width=width, total=total)
    barrier = pltpu.get_barrier_semaphore()

    def up(k):
        return lax.rem(me + k, R)

    def down(k):
        return lax.rem(me - k + R, R)

    def gup(k):
        return lax.rem(mg + k, G)

    def nth_chunk(n):
        return lax.rem(my_chunk + ORDER[n], CHUNKS)

    def exchange(make, send, recv, ss, rs, target):
        used = pl.ds(0, sent)

        def copy(k):
            return pltpu.make_async_remote_copy(
                send.at[target(k), used], recv.at[me, used], ss.at[k], rs.at[me],
                device_id={"rows": target(k)}, device_id_type=pl.DeviceIdType.MESH,
            )

        def arrival(src):
            return pltpu.make_async_remote_copy(
                send.at[src, used], recv.at[src, used], ss.at[0], rs.at[src],
                device_id={"rows": src}, device_id_type=pl.DeviceIdType.MESH,
            )

        def start():
            @pl.loop(1, R)
            def _(k):
                make(target(k))
                copy(k).start()

            make(me)
            recv[me] = send[me]

        def wait_chunk(n):
            if n == 0:
                @pl.loop(1, fan)
                def _(i):
                    arrival(my_chunk * fan + lax.rem(side_of + i, fan)).wait_recv()
            else:
                @pl.loop(0, fan)
                def _(i):
                    arrival(nth_chunk(n) * fan + i).wait_recv()

        def drain():
            @pl.loop(1, R)
            def _(k):
                copy(k).wait_send()

        return start, wait_chunk, drain

    @pl.loop(1, R)
    def _(k):
        pl.semaphore_signal(barrier, inc=1, device_id={"rows": up(k)})

    @pl.loop(1, G)
    def _(k):
        pl.semaphore_signal(barrier, inc=1, device_id={"grp": gup(k)})

    tab_copy = pltpu.make_async_copy(tab_hbm, tab, local_sem.at[0])
    w_copy = pltpu.make_async_copy(w_hbm, w, local_sem.at[1])
    tab_copy.start()
    w_copy.start()

    for ref in (rows, g_recv):
        ref[:, total - 16 : total] = jnp.zeros((R, 16, emb), BF16)
    idx_ref[...] = jnp.zeros_like(idx_ref)
    idx_ref[2:3, 0:bdev] = lab_ref[...]
    for t in range(3):
        for f in range(fgrp):
            lanes = pl.ds(t * per + f * bdev, bdev)
            owner = own_ref[f, t : t + 1, :]
            idx_ref[0:1, lanes] = owner * 8 + t
            idx_ref[1:2, lanes] = off_ref[f, t : t + 1, :]
            idx_ref[3:4, lanes] = owner * width + (t * (cap // 3) - starts[t])
    for j in range(nl // 128):
        col[pl.ds(j * 128, 128), :] = idx_ref[:, pl.ds(j * 128, 128)].T
    for t in range(3):
        at = pl.ds(t * per, per)
        of[at, :] = ones_where(iota((per, n_rows), 1) == col[at, 1:2])
    owner_hot = ones_where(iota((r8, nl), 0) == idx_ref[0:1, :])
    present = mm(owner_hot, of[...]) > 0.5
    before = ones_where(iota((n_rows, n_rows), 0) < iota((n_rows, n_rows), 1))
    ranked = jnp.where(present, mm(ones_where(present), before), -1.0)
    ranked_bf[...] = ranked.astype(BF16)
    req_send[...] = ranked.reshape(R, 8, n_rows)[:, 0:4].astype(BF16)

    pl.semaphore_wait(barrier, R - 1 + G - 1)

    def req_copy(k):
        return pltpu.make_async_remote_copy(
            req_send.at[up(k)], req_recv.at[me], ss0.at[k], rs0.at[me],
            device_id={"rows": up(k)}, device_id_type=pl.DeviceIdType.MESH,
        )

    def req_arrival(src):
        return pltpu.make_async_remote_copy(
            req_send.at[src], req_recv.at[src], ss0.at[0], rs0.at[src],
            device_id={"rows": src}, device_id_type=pl.DeviceIdType.MESH,
        )

    @pl.loop(1, R)
    def _(k):
        req_copy(k).start()

    tab_copy.wait()
    tb[...] = tab[...].astype(BF16)
    req_recv[me] = req_send[me]

    for t in range(3):
        at = pl.ds(t * per, per)
        own_hot = ones_where(iota((per, r8), 1) == col[at, 0:1])
        picked = mm(own_hot, ranked_bf[...]) * of[at, :].astype(F32)
        slot = jnp.sum(picked, axis=1, keepdims=True) + col[at, 3:4].astype(F32)
        looked[t] = jnp.broadcast_to(slot, (per, emb))

    def fetch(src):
        @pl.when(src != me)
        def _():
            req_arrival(src).wait_recv()

        rank = req_recv[src].astype(F32)
        bands = []
        for t in range(3):
            shift = t * (cap // 3) - starts[t]
            line = (iota((width, n_rows), 0) - shift).astype(F32)
            line = jnp.where(line < 0.0, -2.0, line)
            bands.append(mm(ones_where(line == rank[t : t + 1, :]), tb[t]))
        fet_send[src] = joined(bands)

    rows_start, rows_wait, rows_drain = exchange(fetch, fet_send, rows, ss1, rs1, down)
    rows_start()

    lane_slot = iota((per, chunk), 1).astype(F32)
    slot_rows = []
    for t in range(3):
        slot = looked[t]
        for c in range(CHUNKS):
            p_ref[t, c] = ones_where(lane_slot == slot[:, 0:1] - float(c * chunk))
        slot_rows.append(slot.T[0:1, :])
    for t in range(3):
        pt_ref[t] = ones_where(iota((slots, per), 0).astype(F32) == slot_rows[t])
    req_cols = req_recv[...].astype(F32).reshape(R * 4, n_rows).T.astype(BF16)
    row_i = iota((R * 4, chunk), 0)
    slot_in = iota((n_rows, chunk), 1) & (width - 1)
    for t in range(3):
        line = (slot_in - (t * (cap // 3) - starts[t])).astype(F32)
        line = jnp.where(line < 0.0, -2.0, line)
        for c in range(CHUNKS):
            col_j = iota((R * 4, chunk), 1) + c * chunk
            first = (row_i >> 2) * width
            spread = ones_where(((row_i & 3) == t) & (col_j >= first) & (col_j < first + width))
            st_ref[t, c] = ones_where(mm(req_cols, spread) == line)

    def arrived(ref, n, t):
        src = pl.ds(nth_chunk(n) * fan, fan)
        return ref[src, starts[t] : starts[t] + width].reshape(chunk, emb)

    for n in range(CHUNKS):
        rows_wait(n)
        for t in range(3):
            part = mm(p_ref[t, nth_chunk(n)], arrived(rows, n, t))
            looked[t] = part if n == 0 else looked[t] + part
    embedded = (looked[0] * looked[1] + looked[2]).astype(BF16)
    features = jnp.concatenate(
        [embedded[f * bdev : (f + 1) * bdev] for f in range(fgrp)], axis=1
    )
    w_copy.wait()
    partial = mm(features, w[...])
    hidden = partial.shape[1]
    half = G // 2
    side = lax.rem(mg, 2)
    partner = mg + 1 - 2 * side
    mine = lax.div(mg, 2)
    for g in range(G):
        block = partial[g * share : (g + 1) * share]
        part_f32[g % 2, g // 2] = block
        part_send[g % 2, g // 2] = block.astype(BF16)
    swap = pltpu.make_async_remote_copy(
        part_send.at[1 - side], swap_recv, ssp.at[0], rsp.at[0],
        device_id={"grp": partner}, device_id_type=pl.DeviceIdType.MESH,
    )
    swap.start()

    def part_copy(k):
        peer = lax.rem(mg + 2 * k, G)
        return pltpu.make_async_remote_copy(
            pair_send, pair_recv.at[k], ssp.at[k], rsp.at[k],
            device_id={"grp": peer}, device_id_type=pl.DeviceIdType.MESH,
        )

    swap.wait_recv()
    pair = part_f32[side] + swap_recv[...].astype(F32)
    pair_send[...] = pair.astype(BF16)
    for k in range(1, half):
        part_copy(k).start()
    pair = pair + b_ref[...]
    for k in range(1, half):
        part_copy(k).wait_recv()
        pair = pair + pair_recv[k].astype(F32)
    pre = pair.reshape(half * share, hidden)
    sig = jax.nn.sigmoid(pre)
    w_out = wo_ref[...]
    logits = jnp.sum(pre * sig * w_out, axis=1, keepdims=True)
    targets = jnp.concatenate(
        [
            col[pl.ds(pl.multiple_of((2 * j + side) * share, share), share), 2:3]
            for j in range(half)
        ],
        axis=0,
    ).astype(F32)
    grad_logit = jax.nn.sigmoid(logits) - targets
    grad_half = (grad_logit * w_out * (sig * (1.0 + pre * (1.0 - sig)))).astype(BF16)
    gp[side] = grad_half.reshape(half, share, hidden)
    gp_copy = pltpu.make_async_remote_copy(
        gp.at[side], gp.at[side], ssg.at[0], rsg.at[0],
        device_id={"grp": partner}, device_id_type=pl.DeviceIdType.MESH,
    )
    gp_copy.start()
    losses = (
        jnp.maximum(logits, 0.0) + jnp.log1p(jnp.exp(-jnp.abs(logits))) - targets * logits
    )
    diag = iota((half * share, share), 0) - mine * share == iota((half * share, share), 1)
    loss_ref[...] = jnp.sum(jnp.where(diag, losses, 0.0), axis=0, keepdims=True)
    gp_copy.wait_recv()
    grad_pre = jnp.concatenate([gp[g % 2, g // 2] for g in range(G)], axis=0)

    grad_emb = lax.dot_general(
        grad_pre, w[...], (((1,), (1,)), ((), ())),
        preferred_element_type=F32,
    )
    grad_rows = jnp.concatenate(
        [grad_emb[:, f * emb : (f + 1) * emb] for f in range(fgrp)], axis=0
    )
    rg[0] = (grad_rows * looked[1]).astype(BF16)
    rg[1] = (grad_rows * looked[0]).astype(BF16)
    rg[2] = grad_rows.astype(BF16)

    def collect(dst):
        at = pl.ds(pl.multiple_of(dst * width, width), width)
        g_send[dst] = joined([mm(pt_ref[t, at, :], rg[t]) for t in range(3)])

    g_start, g_wait, g_drain = exchange(collect, g_send, g_recv, ss2, rs2, up)
    g_start()

    @pl.loop(1, R)
    def _(k):
        req_copy(k).wait_send()

    rows_drain()
    swap.wait_send()
    gp_copy.wait_send()
    for k in range(1, half):
        part_copy(k).wait_send()

    for n in range(CHUNKS):
        g_wait(n)
        for t in range(3):
            part = mm(st_ref[t, nth_chunk(n)], arrived(g_recv, n, t))
            tg_ref[t] = part if n == 0 else tg_ref[t] + part

    g_drain()


def body(owner, offset, tables, w_first, b_first, w_out, labels):
    R, G = lax.axis_size("rows"), lax.axis_size("grp")
    bdev, fgrp = owner.shape[0], owner.shape[1]
    n_rows, emb = tables.shape[1], tables.shape[2]
    hidden = w_first.shape[1]
    per = bdev * fgrp
    nl = 3 * per
    hot_count = 8 * (per * 7 // (16 * R)) + 8
    uniq = hot_count // 3
    cap = 3 * uniq
    total = -(-cap // 16) * 16
    starts = [t * uniq // 16 * 16 for t in range(3)]
    width = 16
    while any(s + width < (t + 1) * uniq for t, s in enumerate(starts)):
        width *= 2
    total = max(total, max(starts) + width)
    share = bdev // G
    half = G // 2
    slots = R * width

    owner_rows = owner.transpose(1, 2, 0)
    offset_rows = offset.transpose(1, 2, 0)
    vmem = pl.BlockSpec(memory_space=pltpu.VMEM)
    hbm = pl.BlockSpec(memory_space=pl.ANY)
    sems = pltpu.SemaphoreType.DMA
    table_grad, losses = pl.pallas_call(
        functools.partial(kernel, R, G, cap, fgrp, starts, width),
        out_shape=(
            jax.ShapeDtypeStruct((3, n_rows, emb), F32),
            jax.ShapeDtypeStruct((1, share), F32),
        ),
        in_specs=[vmem, vmem, vmem, hbm, hbm, vmem, vmem],
        out_specs=(vmem, vmem),
        scratch_shapes=[
            pltpu.VMEM((8, nl), jnp.int32),
            pltpu.VMEM((3, n_rows, emb), F32),
            pltpu.VMEM((3, n_rows, emb), BF16),
            pltpu.VMEM(w_first.shape, BF16),
            pltpu.VMEM((nl, 8), jnp.int32),
            pltpu.VMEM((nl, n_rows), BF16),
            pltpu.VMEM((R * 8, n_rows), BF16),
            pltpu.VMEM((R, 4, n_rows), BF16),
            pltpu.VMEM((R, 4, n_rows), BF16),
            pltpu.VMEM((R, total, emb), BF16),
            pltpu.VMEM((R, total, emb), BF16),
            pltpu.VMEM((3, per, emb), F32),
            pltpu.VMEM((3, CHUNKS, per, slots // CHUNKS), BF16),
            pltpu.VMEM((3, slots, per), BF16),
            pltpu.VMEM((3, CHUNKS, n_rows, slots // CHUNKS), BF16),
            pltpu.VMEM((2, half, share, hidden), F32),
            pltpu.VMEM((2, half, share, hidden), BF16),
            pltpu.VMEM((half, share, hidden), BF16),
            pltpu.VMEM((half, share, hidden), BF16),
            pltpu.VMEM((half, half, share, hidden), BF16),
            pltpu.VMEM((2, half, share, hidden), BF16),
            pltpu.VMEM((3, per, emb), BF16),
            pltpu.VMEM((R, total, emb), BF16),
            pltpu.VMEM((R, total, emb), BF16),
            sems((2,)),
            sems((R,)), sems((R,)), sems((R,)), sems((R,)), sems((R,)), sems((R,)),
            sems((G,)), sems((G,)), sems((G,)), sems((G,)),
        ],
        compiler_params=pltpu.CompilerParams(
            collective_id=0, has_side_effects=True, vmem_limit_bytes=(44 if slots <= 1024 else 60) * MIB
        ),
        name="embed_step",
    )(
        *(
            pltpu.with_memory_space_constraint(v, pltpu.HBM)
            for v in (
                owner_rows, offset_rows, labels.reshape(1, bdev), tables, w_first,
                b_first.reshape(1, hidden), w_out.reshape(1, hidden),
            )
        )
    )
    return table_grad, losses.reshape(share)


def solution(mesh):
    placed = (
        P("rows", "grp", None),
        P("rows", "grp", None),
        P("grp", "rows", None),
        P("grp", None),
        P(),
        P(),
        P("rows"),
    )
    return jax.shard_map(
        body,
        mesh=mesh,
        in_specs=placed,
        out_specs=(P("grp", "rows", None), P(("rows", "grp"))),
        check_vma=False,
    )
```

```python
import functools

import jax
import jax.numpy as jnp
from jax import lax
from jax.experimental import pallas as pl
from jax.experimental.pallas import tpu as pltpu
from jax.sharding import PartitionSpec as P

BF16 = jnp.bfloat16
F32 = jnp.float32
CHUNKS = 4
PARTS = 2
DENSE_AT = 1
MIB = 1024 * 1024


def iota(shape, dim):
    return lax.broadcasted_iota(jnp.int32, shape, dim)


def ones_where(mask):
    return jnp.where(mask, 1.0, 0.0).astype(BF16)


def join_bands(bands, starts, width, total):
    cuts = sorted({0, total, *starts, *(min(s + width, total) for s in starts)})
    pieces = []
    for lo, hi in zip(cuts[:-1], cuts[1:]):
        piece = None
        for band, s in zip(bands, starts):
            if s <= lo and hi <= s + width:
                part = band[lo - s : hi - s]
                piece = part if piece is None else piece + part
        pieces.append(piece)
    return jnp.concatenate(pieces, axis=0).astype(BF16)


def mm(a, b):
    return jnp.dot(a, b, preferred_element_type=F32)


def kernel(
    R, G, cap, fgrp, starts, width,
    own_ref, off_ref, lab_ref, tab_hbm, w_hbm, b_ref, wo_ref,
    tg_ref, loss_ref,
    idx_ref, tab, tb, w, w_t, col, of, ranked_bf, req_send, req_recv, fet_send, rows, dense, dense_part, looked,
    p_ref, pt_ref, st_ref, part_f32, part_send, swap_recv, pair_send, pair_recv, gp, rg, g_send, g_recv,
    local_sem, ss0, rs0, ss1, rs1, ss2, rs2, ssd, rsd, ssp, rsp, ssg, rsg,
):
    me = lax.axis_index("rows")
    mg = lax.axis_index("grp")
    n_rows = tab.shape[1]
    emb = tab.shape[2]
    nl = idx_ref.shape[1]
    per = nl // 3
    bdev = per // fgrp
    share = bdev // G
    r8 = R * 8
    slots = R * width
    fan = R // CHUNKS
    chunk = fan * width
    my_chunk = lax.div(me, fan)
    side_of = lax.rem(me, fan)
    sent = -(-cap // 8) * 8
    sent_short = starts[1] + width

    total = fet_send.shape[1]
    joined = functools.partial(join_bands, starts=starts, width=width, total=total)
    barrier = pltpu.get_barrier_semaphore()

    def up(k):
        return lax.rem(me + k, R)

    def gup(k):
        return lax.rem(mg + k, G)

    paired = R == 2 * CHUNKS
    my_half = lax.div(my_chunk, 2)
    pair_chunk = my_chunk + 1 - 2 * lax.rem(my_chunk, 2)
    far_inner = 2 - my_half

    def nth_chunk(n):
        if not paired:
            return lax.rem(my_chunk + n, CHUNKS)
        return (my_chunk, pair_chunk, 3 - 3 * my_half, far_inner)[n]

    def is_inner(z):
        return lax.rem(lax.div(z + 1, 2), 2)

    def same(a, b):
        return (a == b).astype(jnp.int32)

    def served(z, y, to_z, to_y):
        across = 1 - same(lax.div(z, 2), lax.div(to_z, 2))
        return is_inner(z) * across * (is_inner(to_z) + (1 - is_inner(to_z)) * same(y, to_y))

    inner = is_inner(my_chunk)

    def exchange(make, send, recv, ss, rs, shorter):
        def copy(k, count):
            return pltpu.make_async_remote_copy(
                send.at[up(k), pl.ds(0, count)], recv.at[me, pl.ds(0, count)], ss.at[k], rs.at[me],
                device_id={"rows": up(k)}, device_id_type=pl.DeviceIdType.MESH,
            )

        def arrival(src, count):
            return pltpu.make_async_remote_copy(
                send.at[src, pl.ds(0, count)], recv.at[src, pl.ds(0, count)], ss.at[0], rs.at[src],
                device_id={"rows": src}, device_id_type=pl.DeviceIdType.MESH,
            )

        def by_size(k, act):
            if not shorter:
                act(copy(k, sent))
                return
            cut = served(my_chunk, side_of, lax.div(up(k), fan), lax.rem(up(k), fan))

            @pl.when(cut == 1)
            def _():
                act(copy(k, sent_short))

            @pl.when(cut == 0)
            def _():
                act(copy(k, sent))

        def start():
            @pl.loop(1, R)
            def _(k):
                make(up(k))
                by_size(k, lambda c: c.start())

            make(me)
            recv[me] = send[me]

        def wait_chunk(n):
            mixed = shorter and n == CHUNKS - 1

            @pl.loop(0, fan)
            def _(i):
                src = nth_chunk(n) * fan + i

                @pl.when(src != me)
                def _():
                    if not mixed:
                        arrival(src, sent).wait_recv()
                        return
                    cut = served(nth_chunk(n), i, my_chunk, side_of)

                    @pl.when(cut == 1)
                    def _():
                        arrival(src, sent_short).wait_recv()

                    @pl.when(cut == 0)
                    def _():
                        arrival(src, sent).wait_recv()

        def drain():
            @pl.loop(1, R)
            def _(k):
                by_size(k, lambda c: c.wait_send())

        return start, wait_chunk, drain

    def dense_copy(j):
        dst = (
            far_inner * fan + side_of,
            my_chunk * fan + 1 - side_of,
            pair_chunk * fan + side_of,
        )[j]
        return pltpu.make_async_remote_copy(
            tb.at[2] if j == 0 else dense.at[side_of], dense.at[side_of], ssd.at[j], rsd.at[side_of],
            device_id={"rows": dst}, device_id_type=pl.DeviceIdType.MESH,
        )

    def dense_wait(ys):
        pltpu.make_async_remote_copy(
            tb.at[2], dense.at[ys], ssd.at[0], rsd.at[ys],
            device_id={"rows": up(1)}, device_id_type=pl.DeviceIdType.MESH,
        ).wait_recv()

    dense[...] = jnp.zeros_like(dense)

    @pl.loop(1, R)
    def _(k):
        pl.semaphore_signal(barrier, inc=1, device_id={"rows": up(k)})

    @pl.loop(1, G)
    def _(k):
        pl.semaphore_signal(barrier, inc=1, device_id={"grp": gup(k)})

    tab_copy = pltpu.make_async_copy(tab_hbm, tab, local_sem.at[0])
    w_copy = pltpu.make_async_copy(w_hbm, w, local_sem.at[1])
    tab_copy.start()
    w_copy.start()

    clear = sent_short if paired else total - 16
    rows[:, clear:total] = jnp.zeros((R, total - clear, emb), BF16)
    g_recv[:, total - 16 : total] = jnp.zeros((R, 16, emb), BF16)
    idx_ref[...] = jnp.zeros_like(idx_ref)
    idx_ref[2:3, 0:bdev] = lab_ref[...]
    for t in range(3):
        for f in range(fgrp):
            lanes = pl.ds(t * per + f * bdev, bdev)
            owner = own_ref[f, t : t + 1, :]
            idx_ref[0:1, lanes] = owner * 8 + t
            idx_ref[1:2, lanes] = off_ref[f, t : t + 1, :]
            idx_ref[3:4, lanes] = owner * width + (t * (cap // 3) - starts[t])
    for j in range(nl // 128):
        col[pl.ds(j * 128, 128), :] = idx_ref[:, pl.ds(j * 128, 128)].T
    for t in range(3):
        at = pl.ds(t * per, per)
        of[at, :] = ones_where(iota((per, n_rows), 1) == col[at, 1:2])
    owner_hot = ones_where(iota((r8, nl), 0) == idx_ref[0:1, :])
    present = mm(owner_hot, of[...]) > 0.5
    before = ones_where(iota((n_rows, n_rows), 0) < iota((n_rows, n_rows), 1))
    ranked = jnp.where(present, mm(ones_where(present), before), -1.0)
    ranked_bf[...] = ranked.astype(BF16)
    req_send[...] = ranked.reshape(R, 8, n_rows)[:, 0:4].astype(BF16)

    pl.semaphore_wait(barrier, R - 1 + G - 1)

    def req_copy(k):
        return pltpu.make_async_remote_copy(
            req_send.at[up(k)], req_recv.at[me], ss0.at[k], rs0.at[me],
            device_id={"rows": up(k)}, device_id_type=pl.DeviceIdType.MESH,
        )

    def req_arrival(src):
        return pltpu.make_async_remote_copy(
            req_send.at[src], req_recv.at[src], ss0.at[0], rs0.at[src],
            device_id={"rows": src}, device_id_type=pl.DeviceIdType.MESH,
        )

    @pl.loop(1, R)
    def _(k):
        req_copy(k).start()

    tab_copy.wait()
    tb[...] = tab[...].astype(BF16)
    if paired:
        @pl.when(inner == 1)
        def _():
            dense_copy(0).start()

    req_recv[me] = req_send[me]

    def fetch(src):
        @pl.when(src != me)
        def _():
            req_arrival(src).wait_recv()

        rank = req_recv[src].astype(F32)
        bands = []
        for t in range(3):
            shift = t * (cap // 3) - starts[t]
            line = (iota((width, n_rows), 0) - shift).astype(F32)
            line = jnp.where(line < 0.0, -2.0, line)
            bands.append(mm(ones_where(line == rank[t : t + 1, :]), tb[t]))
        fet_send[src] = joined(bands)

    rows_start, rows_wait, rows_drain = exchange(fetch, fet_send, rows, ss1, rs1, paired)
    rows_start()
    if paired:
        @pl.when(inner == 1)
        def _():
            dense_wait(side_of)
            for j in range(1, 3):
                dense_copy(j).start()

    for t in range(3):
        at = pl.ds(t * per, per)
        own_hot = ones_where(iota((per, r8), 1) == col[at, 0:1])
        picked = mm(own_hot, ranked_bf[...]) * of[at, :].astype(F32)
        slot = jnp.sum(picked, axis=1, keepdims=True) + col[at, 3:4].astype(F32)
        looked[t] = jnp.broadcast_to(slot, (per, emb))

    lane_slot = iota((per, chunk), 1).astype(F32)
    slot_rows = []
    for t in range(3):
        slot = looked[t]
        for c in range(CHUNKS):
            p_ref[t, c] = ones_where(lane_slot == slot[:, 0:1] - float(c * chunk))
        slot_rows.append(slot.T[0:1, :])
    for t in range(3):
        pt_ref[t] = ones_where(iota((slots, per), 0).astype(F32) == slot_rows[t])
    req_cols = req_recv[...].astype(F32).reshape(R * 4, n_rows).T.astype(BF16)
    row_i = iota((R * 4, chunk), 0)
    slot_in = iota((n_rows, chunk), 1) & (width - 1)
    for t in range(3):
        line = (slot_in - (t * (cap // 3) - starts[t])).astype(F32)
        line = jnp.where(line < 0.0, -2.0, line)
        for c in range(CHUNKS):
            col_j = iota((R * 4, chunk), 1) + c * chunk
            first = (row_i >> 2) * width
            spread = ones_where(((row_i & 3) == t) & (col_j >= first) & (col_j < first + width))
            st_ref[t, c] = ones_where(mm(req_cols, spread) == line)

    w_copy.wait()
    for f in range(fgrp):
        w_t[:, f * emb : (f + 1) * emb] = w[f * emb : (f + 1) * emb, :].T

    def arrived(ref, n, t):
        src = pl.ds(nth_chunk(n) * fan, fan)
        return ref[src, starts[t] : starts[t] + width].reshape(chunk, emb)

    for n in range(CHUNKS):
        rows_wait(n)
        for t in range(3):
            part = mm(p_ref[t, nth_chunk(n)], arrived(rows, n, t))
            looked[t] = part if n == 0 else looked[t] + part
        if paired and n == DENSE_AT:
            at = pl.ds(2 * per, per)
            keys = []
            for ys in range(2):
                used = served(far_inner, ys, my_chunk, side_of)

                @pl.when(used * (1 - inner * same(side_of, ys)) == 1)
                def _():
                    dense_wait(ys)

                key = ((far_inner * fan + ys) * 8 + 2) * used - (1 - used)
                keys.append(key)
                part = jnp.where(col[at, 0:1] == key, mm(of[at, :], dense[ys]), 0.0)
                dense_part[...] = part if ys == 0 else dense_part[...] + part
    if paired:
        hit = (col[at, 0:1] == keys[0]) | (col[at, 0:1] == keys[1])
        looked[2] = jnp.where(hit, dense_part[...], looked[2])
    embedded = (looked[0] * looked[1] + looked[2]).astype(BF16)
    features = jnp.concatenate(
        [embedded[f * bdev : (f + 1) * bdev] for f in range(fgrp)], axis=1
    )
    hidden = w.shape[1]
    half = G // 2
    side = lax.rem(mg, 2)
    partner = mg + 1 - 2 * side
    mine = lax.div(mg, 2)

    def swap(c):
        return pltpu.make_async_remote_copy(
            part_send.at[c, 1 - side], swap_recv.at[c], ssp.at[c], rsp.at[c],
            device_id={"grp": partner}, device_id_type=pl.DeviceIdType.MESH,
        )

    def part_copy(k, c):
        return pltpu.make_async_remote_copy(
            pair_send.at[c], pair_recv.at[k, c], ssp.at[k * PARTS + c], rsp.at[k * PARTS + c],
            device_id={"grp": lax.rem(mg + 2 * k, G)}, device_id_type=pl.DeviceIdType.MESH,
        )

    def gp_copy(c):
        return pltpu.make_async_remote_copy(
            gp.at[c, side], gp.at[c, side], ssg.at[c], rsg.at[c],
            device_id={"grp": partner}, device_id_type=pl.DeviceIdType.MESH,
        )

    piece = hidden // PARTS
    for c in range(PARTS):
        partial = mm(features, w[:, c * piece : (c + 1) * piece])
        for g in range(G):
            block = partial[g * share : (g + 1) * share]
            part_f32[c, g % 2, g // 2] = block
            part_send[c, g % 2, g // 2] = block.astype(BF16)
        swap(c).start()
    for c in range(PARTS):
        swap(c).wait_recv()
        pair = part_f32[c, side] + swap_recv[c].astype(F32)
        pair_send[c] = pair.astype(BF16)
        for k in range(1, half):
            part_copy(k, c).start()
        part_f32[c, side] = pair + b_ref[:, c * piece : (c + 1) * piece]
    logits = jnp.zeros((half * share, 1), F32)
    slopes = []
    for c in range(PARTS):
        pre = part_f32[c, side]
        for k in range(1, half):
            part_copy(k, c).wait_recv()
            pre = pre + pair_recv[k, c].astype(F32)
        pre = pre.reshape(half * share, piece)
        sig = jax.nn.sigmoid(pre)
        w_out = wo_ref[:, c * piece : (c + 1) * piece]
        logits = logits + jnp.sum(pre * sig * w_out, axis=1, keepdims=True)
        slopes.append(w_out * (sig * (1.0 + pre * (1.0 - sig))))
    targets = jnp.concatenate(
        [
            col[pl.ds(pl.multiple_of((2 * j + side) * share, share), share), 2:3]
            for j in range(half)
        ],
        axis=0,
    ).astype(F32)
    grad_logit = jax.nn.sigmoid(logits) - targets
    for c in range(PARTS):
        gp[c, side] = (grad_logit * slopes[c]).astype(BF16).reshape(half, share, piece)
        gp_copy(c).start()
    losses = (
        jnp.maximum(logits, 0.0) + jnp.log1p(jnp.exp(-jnp.abs(logits))) - targets * logits
    )
    diag = iota((half * share, share), 0) - mine * share == iota((half * share, share), 1)
    loss_ref[...] = jnp.sum(jnp.where(diag, losses, 0.0), axis=0, keepdims=True)

    grad_emb = None
    for c in range(PARTS):
        gp_copy(c).wait_recv()
        grad_pre = jnp.concatenate([gp[c, g % 2, g // 2] for g in range(G)], axis=0)
        term = mm(grad_pre, w_t[c * piece : (c + 1) * piece, :])
        grad_emb = term if grad_emb is None else grad_emb + term
    for f in range(fgrp):
        at = pl.ds(f * bdev, bdev)
        grad_rows = grad_emb[:, f * emb : (f + 1) * emb]
        rg[0, at, :] = (grad_rows * looked[1, at, :]).astype(BF16)
        rg[1, at, :] = (grad_rows * looked[0, at, :]).astype(BF16)
        rg[2, at, :] = grad_rows.astype(BF16)

    def collect(dst):
        at = pl.ds(pl.multiple_of(dst * width, width), width)
        g_send[dst] = joined([mm(pt_ref[t, at, :], rg[t]) for t in range(3)])

    g_start, g_wait, g_drain = exchange(collect, g_send, g_recv, ss2, rs2, False)
    g_start()

    @pl.loop(1, R)
    def _(k):
        req_copy(k).wait_send()

    rows_drain()
    if paired:
        @pl.when(inner == 1)
        def _():
            for j in range(3):
                dense_copy(j).wait_send()

    for c in range(PARTS):
        swap(c).wait_send()
        gp_copy(c).wait_send()
        for k in range(1, half):
            part_copy(k, c).wait_send()

    for n in range(CHUNKS):
        g_wait(n)
        for t in range(3):
            part = mm(st_ref[t, nth_chunk(n)], arrived(g_recv, n, t))
            tg_ref[t] = part if n == 0 else tg_ref[t] + part

    g_drain()


def store(tg_ref, loss_ref, tg_out, loss_out, sem):
    copies = (
        pltpu.make_async_copy(tg_ref, tg_out, sem.at[0]),
        pltpu.make_async_copy(loss_ref, loss_out, sem.at[1]),
    )
    for copy in copies:
        copy.start()
    for copy in copies:
        copy.wait()


def body(owner, offset, tables, w_first, b_first, w_out, labels):
    R, G = lax.axis_size("rows"), lax.axis_size("grp")
    bdev, fgrp = owner.shape[0], owner.shape[1]
    n_rows, emb = tables.shape[1], tables.shape[2]
    hidden = w_first.shape[1]
    per = bdev * fgrp
    nl = 3 * per
    hot_count = 8 * (per * 7 // (16 * R)) + 8
    uniq = hot_count // 3
    cap = 3 * uniq
    total = -(-cap // 16) * 16
    starts = [t * uniq // 16 * 16 for t in range(3)]
    width = 16
    while any(s + width < (t + 1) * uniq for t, s in enumerate(starts)):
        width *= 2
    total = max(total, max(starts) + width)
    share = bdev // G
    half = G // 2
    slots = R * width
    piece = hidden // PARTS

    owner_rows = owner.transpose(1, 2, 0)
    offset_rows = offset.transpose(1, 2, 0)
    vmem = pl.BlockSpec(memory_space=pltpu.VMEM)
    hbm = pl.BlockSpec(memory_space=pl.ANY)
    sems = pltpu.SemaphoreType.DMA
    table_grad, losses = pl.pallas_call(
        functools.partial(kernel, R, G, cap, fgrp, starts, width),
        out_shape=(
            jax.ShapeDtypeStruct((3, n_rows, emb), F32),
            jax.ShapeDtypeStruct((1, share), F32),
        ),
        in_specs=[vmem, vmem, vmem, hbm, hbm, vmem, vmem],
        out_specs=(vmem, vmem),
        scratch_shapes=[
            pltpu.VMEM((8, nl), jnp.int32),
            pltpu.VMEM((3, n_rows, emb), F32),
            pltpu.VMEM((3, n_rows, emb), BF16),
            pltpu.VMEM(w_first.shape, BF16),
            pltpu.VMEM((hidden, fgrp * emb), BF16),
            pltpu.VMEM((nl, 8), jnp.int32),
            pltpu.VMEM((nl, n_rows), BF16),
            pltpu.VMEM((R * 8, n_rows), BF16),
            pltpu.VMEM((R, 4, n_rows), BF16),
            pltpu.VMEM((R, 4, n_rows), BF16),
            pltpu.VMEM((R, total, emb), BF16),
            pltpu.VMEM((R, total, emb), BF16),
            pltpu.VMEM((2, n_rows if R == 2 * CHUNKS else 16, emb), BF16),
            pltpu.VMEM((per if R == 2 * CHUNKS else 8, emb), F32),
            pltpu.VMEM((3, per, emb), F32),
            pltpu.VMEM((3, CHUNKS, per, slots // CHUNKS), BF16),
            pltpu.VMEM((3, slots, per), BF16),
            pltpu.VMEM((3, CHUNKS, n_rows, slots // CHUNKS), BF16),
            pltpu.VMEM((PARTS, 2, half, share, piece), F32),
            pltpu.VMEM((PARTS, 2, half, share, piece), BF16),
            pltpu.VMEM((PARTS, half, share, piece), BF16),
            pltpu.VMEM((PARTS, half, share, piece), BF16),
            pltpu.VMEM((half, PARTS, half, share, piece), BF16),
            pltpu.VMEM((PARTS, 2, half, share, piece), BF16),
            pltpu.VMEM((3, per, emb), BF16),
            pltpu.VMEM((R, total, emb), BF16),
            pltpu.VMEM((R, total, emb), BF16),
            sems((2,)),
            sems((R,)), sems((R,)), sems((R,)), sems((R,)), sems((R,)), sems((R,)),
            sems((4,)), sems((2,)),
            sems((half * PARTS,)), sems((half * PARTS,)), sems((PARTS,)), sems((PARTS,)),
        ],
        compiler_params=pltpu.CompilerParams(
            collective_id=0, has_side_effects=True, vmem_limit_bytes=(44 if slots <= 1024 else 60) * MIB
        ),
        name="embed_step",
    )(
        *(
            pltpu.with_memory_space_constraint(v, pltpu.HBM)
            for v in (
                owner_rows, offset_rows, labels.reshape(1, bdev), tables, w_first,
                b_first.reshape(1, hidden), w_out.reshape(1, hidden),
            )
        )
    )
    table_grad, losses = pl.pallas_call(
        store,
        out_shape=(
            jax.ShapeDtypeStruct((3, n_rows, emb), F32),
            jax.ShapeDtypeStruct((1, share), F32),
        ),
        in_specs=[vmem, vmem],
        out_specs=(hbm, hbm),
        scratch_shapes=[sems((2,))],
        compiler_params=pltpu.CompilerParams(vmem_limit_bytes=MIB),
        name="store",
    )(table_grad, losses)
    return table_grad, losses.reshape(share)


def solution(mesh):
    placed = (
        P("rows", "grp", None),
        P("rows", "grp", None),
        P("grp", "rows", None),
        P("grp", None),
        P(),
        P(),
        P("rows"),
    )
    return jax.shard_map(
        body,
        mesh=mesh,
        in_specs=placed,
        out_specs=(P("grp", "rows", None), P(("rows", "grp"))),
        check_vma=False,
    )
```

```python
import functools

import jax
import jax.numpy as jnp
from jax import lax
from jax.experimental import pallas as pl
from jax.experimental.pallas import tpu as pltpu
from jax.sharding import PartitionSpec as P

BF16 = jnp.bfloat16
F32 = jnp.float32
CHUNKS = 4
PARTS = 1
DENSE_AT = 2
MIB = 1024 * 1024


def iota(shape, dim):
    return lax.broadcasted_iota(jnp.int32, shape, dim)


def ones_where(mask):
    return jnp.where(mask, 1.0, 0.0).astype(BF16)


def join_bands(bands, starts, width, total):
    cuts = sorted({0, total, *starts, *(min(s + width, total) for s in starts)})
    pieces = []
    for lo, hi in zip(cuts[:-1], cuts[1:]):
        piece = None
        for band, s in zip(bands, starts):
            if s <= lo and hi <= s + width:
                part = band[lo - s : hi - s]
                piece = part if piece is None else piece + part
        pieces.append(piece)
    return jnp.concatenate(pieces, axis=0).astype(BF16)


def mm(a, b):
    return jnp.dot(a, b, preferred_element_type=F32)


def kernel(
    R, G, cap, fgrp, starts, width,
    own_ref, off_ref, lab_ref, tab_hbm, w_hbm, b_ref, wo_ref,
    tg_ref, loss_ref,
    idx_ref, tab, tb, w, w_t, col, of, ranked_bf, req_send, req_recv, fet_send, rows, dense, dense_part, looked,
    p_ref, pt_ref, st_ref, part_f32, part_send, swap_recv, pair_send, pair_recv, gp, rg, g_send, g_recv,
    local_sem, ss0, rs0, ss1, rs1, ss2, rs2, ssd, rsd, ssp, rsp, ssg, rsg,
):
    me = lax.axis_index("rows")
    mg = lax.axis_index("grp")
    n_rows = tab.shape[1]
    emb = tab.shape[2]
    nl = idx_ref.shape[1]
    per = nl // 3
    bdev = per // fgrp
    share = bdev // G
    r8 = R * 8
    slots = R * width
    fan = R // CHUNKS
    chunk = fan * width
    my_chunk = lax.div(me, fan)
    side_of = lax.rem(me, fan)
    sent = -(-cap // 8) * 8
    sent_short = starts[1] + width

    total = fet_send.shape[1]
    joined = functools.partial(join_bands, starts=starts, width=width, total=total)
    barrier = pltpu.get_barrier_semaphore()

    def up(k):
        return lax.rem(me + k, R)

    def gup(k):
        return lax.rem(mg + k, G)

    paired = R == 2 * CHUNKS
    my_half = lax.div(my_chunk, 2)
    pair_chunk = my_chunk + 1 - 2 * lax.rem(my_chunk, 2)
    far_inner = 2 - my_half

    def nth_chunk(n):
        if not paired:
            return lax.rem(my_chunk + n, CHUNKS)
        return (my_chunk, 3 - 3 * my_half, pair_chunk, far_inner)[n]

    def is_inner(z):
        return lax.rem(lax.div(z + 1, 2), 2)

    def same(a, b):
        return (a == b).astype(jnp.int32)

    def served(z, y, to_z, to_y):
        across = 1 - same(lax.div(z, 2), lax.div(to_z, 2))
        return is_inner(z) * across * (is_inner(to_z) + (1 - is_inner(to_z)) * same(y, to_y))

    inner = is_inner(my_chunk)

    def exchange(make, send, recv, ss, rs, shorter):
        def copy(k, count):
            return pltpu.make_async_remote_copy(
                send.at[up(k), pl.ds(0, count)], recv.at[me, pl.ds(0, count)], ss.at[k], rs.at[me],
                device_id={"rows": up(k)}, device_id_type=pl.DeviceIdType.MESH,
            )

        def arrival(src, count):
            return pltpu.make_async_remote_copy(
                send.at[src, pl.ds(0, count)], recv.at[src, pl.ds(0, count)], ss.at[0], rs.at[src],
                device_id={"rows": src}, device_id_type=pl.DeviceIdType.MESH,
            )

        def by_size(k, act):
            if not shorter:
                act(copy(k, sent))
                return
            cut = served(my_chunk, side_of, lax.div(up(k), fan), lax.rem(up(k), fan))

            @pl.when(cut == 1)
            def _():
                act(copy(k, sent_short))

            @pl.when(cut == 0)
            def _():
                act(copy(k, sent))

        def start():
            @pl.loop(1, R)
            def _(k):
                make(up(k))
                by_size(k, lambda c: c.start())

            make(me)
            recv[me] = send[me]

        def wait_chunk(n):
            mixed = shorter and n == CHUNKS - 1

            @pl.loop(0, fan)
            def _(i):
                src = nth_chunk(n) * fan + i

                @pl.when(src != me)
                def _():
                    if not mixed:
                        arrival(src, sent).wait_recv()
                        return
                    cut = served(nth_chunk(n), i, my_chunk, side_of)

                    @pl.when(cut == 1)
                    def _():
                        arrival(src, sent_short).wait_recv()

                    @pl.when(cut == 0)
                    def _():
                        arrival(src, sent).wait_recv()

        def drain():
            @pl.loop(1, R)
            def _(k):
                by_size(k, lambda c: c.wait_send())

        return start, wait_chunk, drain

    def dense_copy(j):
        dst = (
            far_inner * fan + side_of,
            my_chunk * fan + 1 - side_of,
            pair_chunk * fan + side_of,
        )[j]
        return pltpu.make_async_remote_copy(
            tb.at[2] if j == 0 else dense.at[side_of], dense.at[side_of], ssd.at[j], rsd.at[side_of],
            device_id={"rows": dst}, device_id_type=pl.DeviceIdType.MESH,
        )

    def dense_wait(ys):
        pltpu.make_async_remote_copy(
            tb.at[2], dense.at[ys], ssd.at[0], rsd.at[ys],
            device_id={"rows": up(1)}, device_id_type=pl.DeviceIdType.MESH,
        ).wait_recv()

    dense[...] = jnp.zeros_like(dense)

    @pl.loop(1, R)
    def _(k):
        pl.semaphore_signal(barrier, inc=1, device_id={"rows": up(k)})

    @pl.loop(1, G)
    def _(k):
        pl.semaphore_signal(barrier, inc=1, device_id={"grp": gup(k)})

    tab_copy = pltpu.make_async_copy(tab_hbm, tab, local_sem.at[0])
    w_copy = pltpu.make_async_copy(w_hbm, w, local_sem.at[1])
    tab_copy.start()
    w_copy.start()

    clear = sent_short if paired else total - 16
    rows[:, clear:total] = jnp.zeros((R, total - clear, emb), BF16)
    g_recv[:, total - 16 : total] = jnp.zeros((R, 16, emb), BF16)
    idx_ref[...] = jnp.zeros_like(idx_ref)
    idx_ref[2:3, 0:bdev] = lab_ref[...]
    for t in range(3):
        for f in range(fgrp):
            lanes = pl.ds(t * per + f * bdev, bdev)
            owner = own_ref[f, t : t + 1, :]
            idx_ref[0:1, lanes] = owner * 8 + t
            idx_ref[1:2, lanes] = off_ref[f, t : t + 1, :]
            idx_ref[3:4, lanes] = owner * width + (t * (cap // 3) - starts[t])
    for j in range(nl // 128):
        col[pl.ds(j * 128, 128), :] = idx_ref[:, pl.ds(j * 128, 128)].T
    for t in range(3):
        at = pl.ds(t * per, per)
        of[at, :] = ones_where(iota((per, n_rows), 1) == col[at, 1:2])
    owner_hot = ones_where(iota((r8, nl), 0) == idx_ref[0:1, :])
    present = mm(owner_hot, of[...]) > 0.5
    before = ones_where(iota((n_rows, n_rows), 0) < iota((n_rows, n_rows), 1))
    ranked = jnp.where(present, mm(ones_where(present), before), -1.0)
    ranked_bf[...] = ranked.astype(BF16)
    req_send[...] = ranked.reshape(R, 8, n_rows)[:, 0:4].astype(BF16)

    pl.semaphore_wait(barrier, R - 1 + G - 1)

    def req_copy(k):
        return pltpu.make_async_remote_copy(
            req_send.at[up(k)], req_recv.at[me], ss0.at[k], rs0.at[me],
            device_id={"rows": up(k)}, device_id_type=pl.DeviceIdType.MESH,
        )

    def req_arrival(src):
        return pltpu.make_async_remote_copy(
            req_send.at[src], req_recv.at[src], ss0.at[0], rs0.at[src],
            device_id={"rows": src}, device_id_type=pl.DeviceIdType.MESH,
        )

    @pl.loop(1, R)
    def _(k):
        req_copy(k).start()

    tab_copy.wait()
    tb[...] = tab[...].astype(BF16)
    if paired:
        @pl.when(inner == 1)
        def _():
            dense_copy(0).start()

    req_recv[me] = req_send[me]

    def fetch(src):
        @pl.when(src != me)
        def _():
            req_arrival(src).wait_recv()

        rank = req_recv[src].astype(F32)
        bands = []
        for t in range(3):
            shift = t * (cap // 3) - starts[t]
            line = (iota((width, n_rows), 0) - shift).astype(F32)
            line = jnp.where(line < 0.0, -2.0, line)
            bands.append(mm(ones_where(line == rank[t : t + 1, :]), tb[t]))
        fet_send[src] = joined(bands)

    rows_start, rows_wait, rows_drain = exchange(fetch, fet_send, rows, ss1, rs1, paired)
    rows_start()
    if paired:
        @pl.when(inner == 1)
        def _():
            dense_wait(side_of)
            for j in range(1, 3):
                dense_copy(j).start()

    for t in range(3):
        at = pl.ds(t * per, per)
        own_hot = ones_where(iota((per, r8), 1) == col[at, 0:1])
        picked = mm(own_hot, ranked_bf[...]) * of[at, :].astype(F32)
        slot = jnp.sum(picked, axis=1, keepdims=True) + col[at, 3:4].astype(F32)
        looked[t] = jnp.broadcast_to(slot, (per, emb))

    lane_slot = iota((per, chunk), 1).astype(F32)
    slot_rows = []
    for t in range(3):
        slot = looked[t]
        for c in range(CHUNKS):
            p_ref[t, c] = ones_where(lane_slot == slot[:, 0:1] - float(c * chunk))
        slot_rows.append(slot.T[0:1, :])
    for t in range(3):
        pt_ref[t] = ones_where(iota((slots, per), 0).astype(F32) == slot_rows[t])
    req_cols = req_recv[...].astype(F32).reshape(R * 4, n_rows).T.astype(BF16)
    row_i = iota((R * 4, chunk), 0)
    slot_in = iota((n_rows, chunk), 1) & (width - 1)
    for t in range(3):
        line = (slot_in - (t * (cap // 3) - starts[t])).astype(F32)
        line = jnp.where(line < 0.0, -2.0, line)
        for c in range(CHUNKS):
            col_j = iota((R * 4, chunk), 1) + c * chunk
            first = (row_i >> 2) * width
            spread = ones_where(((row_i & 3) == t) & (col_j >= first) & (col_j < first + width))
            st_ref[t, c] = ones_where(mm(req_cols, spread) == line)

    w_copy.wait()
    for f in range(fgrp):
        w_t[:, f * emb : (f + 1) * emb] = w[f * emb : (f + 1) * emb, :].T

    def arrived(ref, n, t):
        src = pl.ds(nth_chunk(n) * fan, fan)
        return ref[src, starts[t] : starts[t] + width].reshape(chunk, emb)

    for n in range(CHUNKS):
        rows_wait(n)
        for t in range(3):
            part = mm(p_ref[t, nth_chunk(n)], arrived(rows, n, t))
            looked[t] = part if n == 0 else looked[t] + part
        if paired and n == DENSE_AT:
            at = pl.ds(2 * per, per)
            keys = []
            for ys in range(2):
                used = served(far_inner, ys, my_chunk, side_of)

                @pl.when(used * (1 - inner * same(side_of, ys)) == 1)
                def _():
                    dense_wait(ys)

                key = ((far_inner * fan + ys) * 8 + 2) * used - (1 - used)
                keys.append(key)
                part = jnp.where(col[at, 0:1] == key, mm(of[at, :], dense[ys]), 0.0)
                dense_part[...] = part if ys == 0 else dense_part[...] + part
    if paired:
        hit = (col[at, 0:1] == keys[0]) | (col[at, 0:1] == keys[1])
        looked[2] = jnp.where(hit, dense_part[...], looked[2])
    embedded = (looked[0] * looked[1] + looked[2]).astype(BF16)
    features = jnp.concatenate(
        [embedded[f * bdev : (f + 1) * bdev] for f in range(fgrp)], axis=1
    )
    hidden = w.shape[1]
    half = G // 2
    side = lax.rem(mg, 2)
    partner = mg + 1 - 2 * side
    mine = lax.div(mg, 2)

    def swap(c):
        return pltpu.make_async_remote_copy(
            part_send.at[c, 1 - side], swap_recv.at[c], ssp.at[c], rsp.at[c],
            device_id={"grp": partner}, device_id_type=pl.DeviceIdType.MESH,
        )

    def part_copy(k, c):
        return pltpu.make_async_remote_copy(
            pair_send.at[c], pair_recv.at[k, c], ssp.at[k * PARTS + c], rsp.at[k * PARTS + c],
            device_id={"grp": lax.rem(mg + 2 * k, G)}, device_id_type=pl.DeviceIdType.MESH,
        )

    def gp_copy(c):
        return pltpu.make_async_remote_copy(
            gp.at[c, side], gp.at[c, side], ssg.at[c], rsg.at[c],
            device_id={"grp": partner}, device_id_type=pl.DeviceIdType.MESH,
        )

    piece = hidden // PARTS
    for c in range(PARTS):
        partial = mm(features, w[:, c * piece : (c + 1) * piece])
        for g in range(G):
            block = partial[g * share : (g + 1) * share]
            part_f32[c, g % 2, g // 2] = block
            part_send[c, g % 2, g // 2] = block.astype(BF16)
        swap(c).start()
    for c in range(PARTS):
        swap(c).wait_recv()
        pair = part_f32[c, side] + swap_recv[c].astype(F32)
        pair_send[c] = pair.astype(BF16)
        for k in range(1, half):
            part_copy(k, c).start()
        part_f32[c, side] = pair + b_ref[:, c * piece : (c + 1) * piece]
    logits = jnp.zeros((half * share, 1), F32)
    slopes = []
    for c in range(PARTS):
        pre = part_f32[c, side]
        for k in range(1, half):
            part_copy(k, c).wait_recv()
            pre = pre + pair_recv[k, c].astype(F32)
        pre = pre.reshape(half * share, piece)
        sig = jax.nn.sigmoid(pre)
        w_out = wo_ref[:, c * piece : (c + 1) * piece]
        logits = logits + jnp.sum(pre * sig * w_out, axis=1, keepdims=True)
        slopes.append(w_out * (sig * (1.0 + pre * (1.0 - sig))))
    targets = jnp.concatenate(
        [
            col[pl.ds(pl.multiple_of((2 * j + side) * share, share), share), 2:3]
            for j in range(half)
        ],
        axis=0,
    ).astype(F32)
    grad_logit = jax.nn.sigmoid(logits) - targets
    for c in range(PARTS):
        gp[c, side] = (grad_logit * slopes[c]).astype(BF16).reshape(half, share, piece)
        gp_copy(c).start()
    losses = (
        jnp.maximum(logits, 0.0) + jnp.log1p(jnp.exp(-jnp.abs(logits))) - targets * logits
    )
    diag = iota((half * share, share), 0) - mine * share == iota((half * share, share), 1)
    loss_ref[...] = jnp.sum(jnp.where(diag, losses, 0.0), axis=0, keepdims=True)

    grad_emb = None
    for c in range(PARTS):
        gp_copy(c).wait_recv()
        grad_pre = jnp.concatenate([gp[c, g % 2, g // 2] for g in range(G)], axis=0)
        term = mm(grad_pre, w_t[c * piece : (c + 1) * piece, :])
        grad_emb = term if grad_emb is None else grad_emb + term
    for f in range(fgrp):
        at = pl.ds(f * bdev, bdev)
        grad_rows = grad_emb[:, f * emb : (f + 1) * emb]
        rg[0, at, :] = (grad_rows * looked[1, at, :]).astype(BF16)
        rg[1, at, :] = (grad_rows * looked[0, at, :]).astype(BF16)
        rg[2, at, :] = grad_rows.astype(BF16)

    def collect(dst):
        at = pl.ds(pl.multiple_of(dst * width, width), width)
        g_send[dst] = joined([mm(pt_ref[t, at, :], rg[t]) for t in range(3)])

    g_start, g_wait, g_drain = exchange(collect, g_send, g_recv, ss2, rs2, False)
    g_start()

    @pl.loop(1, R)
    def _(k):
        req_copy(k).wait_send()

    rows_drain()
    if paired:
        @pl.when(inner == 1)
        def _():
            for j in range(3):
                dense_copy(j).wait_send()

    for c in range(PARTS):
        swap(c).wait_send()
        gp_copy(c).wait_send()
        for k in range(1, half):
            part_copy(k, c).wait_send()

    for n in range(CHUNKS):
        g_wait(n)
        for t in range(3):
            part = mm(st_ref[t, nth_chunk(n)], arrived(g_recv, n, t))
            tg_ref[t] = part if n == 0 else tg_ref[t] + part

    g_drain()


def store(tg_ref, loss_ref, tg_out, loss_out, sem):
    copies = (
        pltpu.make_async_copy(tg_ref, tg_out, sem.at[0]),
        pltpu.make_async_copy(loss_ref, loss_out, sem.at[1]),
    )
    for copy in copies:
        copy.start()
    for copy in copies:
        copy.wait()


def body(owner, offset, tables, w_first, b_first, w_out, labels):
    R, G = lax.axis_size("rows"), lax.axis_size("grp")
    bdev, fgrp = owner.shape[0], owner.shape[1]
    n_rows, emb = tables.shape[1], tables.shape[2]
    hidden = w_first.shape[1]
    per = bdev * fgrp
    nl = 3 * per
    hot_count = 8 * (per * 7 // (16 * R)) + 8
    uniq = hot_count // 3
    cap = 3 * uniq
    total = -(-cap // 16) * 16
    starts = [t * uniq // 16 * 16 for t in range(3)]
    width = 16
    while any(s + width < (t + 1) * uniq for t, s in enumerate(starts)):
        width *= 2
    total = max(total, max(starts) + width)
    share = bdev // G
    half = G // 2
    slots = R * width
    piece = hidden // PARTS

    owner_rows = owner.transpose(1, 2, 0)
    offset_rows = offset.transpose(1, 2, 0)
    vmem = pl.BlockSpec(memory_space=pltpu.VMEM)
    hbm = pl.BlockSpec(memory_space=pl.ANY)
    sems = pltpu.SemaphoreType.DMA
    table_grad, losses = pl.pallas_call(
        functools.partial(kernel, R, G, cap, fgrp, starts, width),
        out_shape=(
            jax.ShapeDtypeStruct((3, n_rows, emb), F32),
            jax.ShapeDtypeStruct((1, share), F32),
        ),
        in_specs=[vmem, vmem, vmem, hbm, hbm, vmem, vmem],
        out_specs=(vmem, vmem),
        scratch_shapes=[
            pltpu.VMEM((8, nl), jnp.int32),
            pltpu.VMEM((3, n_rows, emb), F32),
            pltpu.VMEM((3, n_rows, emb), BF16),
            pltpu.VMEM(w_first.shape, BF16),
            pltpu.VMEM((hidden, fgrp * emb), BF16),
            pltpu.VMEM((nl, 8), jnp.int32),
            pltpu.VMEM((nl, n_rows), BF16),
            pltpu.VMEM((R * 8, n_rows), BF16),
            pltpu.VMEM((R, 4, n_rows), BF16),
            pltpu.VMEM((R, 4, n_rows), BF16),
            pltpu.VMEM((R, total, emb), BF16),
            pltpu.VMEM((R, total, emb), BF16),
            pltpu.VMEM((2, n_rows if R == 2 * CHUNKS else 16, emb), BF16),
            pltpu.VMEM((per if R == 2 * CHUNKS else 8, emb), F32),
            pltpu.VMEM((3, per, emb), F32),
            pltpu.VMEM((3, CHUNKS, per, slots // CHUNKS), BF16),
            pltpu.VMEM((3, slots, per), BF16),
            pltpu.VMEM((3, CHUNKS, n_rows, slots // CHUNKS), BF16),
            pltpu.VMEM((PARTS, 2, half, share, piece), F32),
            pltpu.VMEM((PARTS, 2, half, share, piece), BF16),
            pltpu.VMEM((PARTS, half, share, piece), BF16),
            pltpu.VMEM((PARTS, half, share, piece), BF16),
            pltpu.VMEM((half, PARTS, half, share, piece), BF16),
            pltpu.VMEM((PARTS, 2, half, share, piece), BF16),
            pltpu.VMEM((3, per, emb), BF16),
            pltpu.VMEM((R, total, emb), BF16),
            pltpu.VMEM((R, total, emb), BF16),
            sems((2,)),
            sems((R,)), sems((R,)), sems((R,)), sems((R,)), sems((R,)), sems((R,)),
            sems((4,)), sems((2,)),
            sems((half * PARTS,)), sems((half * PARTS,)), sems((PARTS,)), sems((PARTS,)),
        ],
        compiler_params=pltpu.CompilerParams(
            collective_id=0, has_side_effects=True, vmem_limit_bytes=(44 if slots <= 1024 else 60) * MIB
        ),
        name="embed_step",
    )(
        *(
            pltpu.with_memory_space_constraint(v, pltpu.HBM)
            for v in (
                owner_rows, offset_rows, labels.reshape(1, bdev), tables, w_first,
                b_first.reshape(1, hidden), w_out.reshape(1, hidden),
            )
        )
    )
    table_grad, losses = pl.pallas_call(
        store,
        out_shape=(
            jax.ShapeDtypeStruct((3, n_rows, emb), F32),
            jax.ShapeDtypeStruct((1, share), F32),
        ),
        in_specs=[vmem, vmem],
        out_specs=(hbm, hbm),
        scratch_shapes=[sems((2,))],
        compiler_params=pltpu.CompilerParams(vmem_limit_bytes=MIB),
        name="store",
    )(table_grad, losses)
    return table_grad, losses.reshape(share)


def solution(mesh):
    placed = (
        P("rows", "grp", None),
        P("rows", "grp", None),
        P("grp", "rows", None),
        P("grp", None),
        P(),
        P(),
        P("rows"),
    )
    return jax.shard_map(
        body,
        mesh=mesh,
        in_specs=placed,
        out_specs=(P("grp", "rows", None), P(("rows", "grp"))),
        check_vma=False,
    )
```

```python
import functools

import jax
import jax.numpy as jnp
from jax import lax
from jax.experimental import pallas as pl
from jax.experimental.pallas import tpu as pltpu
from jax.sharding import PartitionSpec as P

BF16 = jnp.bfloat16
F32 = jnp.float32
CHUNKS = 4
PARTS = 1
DENSE_AT = 2
MIB = 1024 * 1024


def iota(shape, dim):
    return lax.broadcasted_iota(jnp.int32, shape, dim)


def ones_where(mask):
    return jnp.where(mask, 1.0, 0.0).astype(BF16)


def join_bands(bands, starts, width, total):
    cuts = sorted({0, total, *starts, *(min(s + width, total) for s in starts)})
    pieces = []
    for lo, hi in zip(cuts[:-1], cuts[1:]):
        piece = None
        for band, s in zip(bands, starts):
            if s <= lo and hi <= s + width:
                part = band[lo - s : hi - s]
                piece = part if piece is None else piece + part
        pieces.append(piece)
    return jnp.concatenate(pieces, axis=0).astype(BF16)


def mm(a, b):
    return jnp.dot(a, b, preferred_element_type=F32)


def kernel(
    R, G, cap, fgrp, starts, width,
    own_ref, off_ref, lab_ref, tab_hbm, w_hbm, b_ref, wo_ref,
    tg_ref, loss_ref,
    idx_ref, tab, tb, w, w_t, col, of, ranked_bf, req_send, req_recv, fet_send, rows, dense, dense_part, looked,
    p_ref, pt_ref, st_ref, part_f32, part_send, swap_recv, pair_send, pair_recv, gp, rg, g_send, g_recv,
    local_sem, ss0, rs0, ss1, rs1, ss2, rs2, ssd, rsd, ssp, rsp, ssg, rsg,
):
    me = lax.axis_index("rows")
    mg = lax.axis_index("grp")
    n_rows = tab.shape[1]
    emb = tab.shape[2]
    nl = idx_ref.shape[1]
    per = nl // 3
    bdev = per // fgrp
    share = bdev // G
    r8 = R * 8
    slots = R * width
    fan = R // CHUNKS
    chunk = fan * width
    my_chunk = lax.div(me, fan)
    side_of = lax.rem(me, fan)
    sent = -(-cap // 8) * 8
    sent_short = starts[1] + width

    total = fet_send.shape[1]
    joined = functools.partial(join_bands, starts=starts, width=width, total=total)
    barrier = pltpu.get_barrier_semaphore()

    def up(k):
        return lax.rem(me + k, R)

    def gup(k):
        return lax.rem(mg + k, G)

    paired = R == 2 * CHUNKS
    my_half = lax.div(my_chunk, 2)
    pair_chunk = my_chunk + 1 - 2 * lax.rem(my_chunk, 2)
    far_inner = 2 - my_half

    def nth_chunk(n):
        if not paired:
            return lax.rem(my_chunk + n, CHUNKS)
        return (my_chunk, 3 - 3 * my_half, pair_chunk, far_inner)[n]

    def is_inner(z):
        return lax.rem(lax.div(z + 1, 2), 2)

    def same(a, b):
        return (a == b).astype(jnp.int32)

    def served(z, y, to_z, to_y):
        across = 1 - same(lax.div(z, 2), lax.div(to_z, 2))
        return is_inner(z) * across * (is_inner(to_z) + (1 - is_inner(to_z)) * same(y, to_y))

    inner = is_inner(my_chunk)

    def exchange(make, send, recv, ss, rs, shorter):
        def copy(k, count):
            return pltpu.make_async_remote_copy(
                send.at[up(k), pl.ds(0, count)], recv.at[me, pl.ds(0, count)], ss.at[k], rs.at[me],
                device_id={"rows": up(k)}, device_id_type=pl.DeviceIdType.MESH,
            )

        def arrival(src, count):
            return pltpu.make_async_remote_copy(
                send.at[src, pl.ds(0, count)], recv.at[src, pl.ds(0, count)], ss.at[0], rs.at[src],
                device_id={"rows": src}, device_id_type=pl.DeviceIdType.MESH,
            )

        def by_size(k, act):
            if not shorter:
                act(copy(k, sent))
                return
            cut = served(my_chunk, side_of, lax.div(up(k), fan), lax.rem(up(k), fan))

            @pl.when(cut == 1)
            def _():
                act(copy(k, sent_short))

            @pl.when(cut == 0)
            def _():
                act(copy(k, sent))

        def start():
            @pl.loop(1, R)
            def _(k):
                make(up(k))
                by_size(k, lambda c: c.start())

            make(me)
            recv[me] = send[me]

        def wait_chunk(n):
            mixed = shorter and n == CHUNKS - 1

            @pl.loop(0, fan)
            def _(i):
                src = nth_chunk(n) * fan + i

                @pl.when(src != me)
                def _():
                    if not mixed:
                        arrival(src, sent).wait_recv()
                        return
                    cut = served(nth_chunk(n), i, my_chunk, side_of)

                    @pl.when(cut == 1)
                    def _():
                        arrival(src, sent_short).wait_recv()

                    @pl.when(cut == 0)
                    def _():
                        arrival(src, sent).wait_recv()

        def drain():
            @pl.loop(1, R)
            def _(k):
                by_size(k, lambda c: c.wait_send())

        return start, wait_chunk, drain

    def dense_copy(j):
        dst = (
            far_inner * fan + side_of,
            my_chunk * fan + 1 - side_of,
            pair_chunk * fan + side_of,
        )[j]
        return pltpu.make_async_remote_copy(
            tb.at[2] if j == 0 else dense.at[side_of], dense.at[side_of], ssd.at[j], rsd.at[side_of],
            device_id={"rows": dst}, device_id_type=pl.DeviceIdType.MESH,
        )

    def dense_wait(ys):
        pltpu.make_async_remote_copy(
            tb.at[2], dense.at[ys], ssd.at[0], rsd.at[ys],
            device_id={"rows": up(1)}, device_id_type=pl.DeviceIdType.MESH,
        ).wait_recv()

    dense[...] = jnp.zeros_like(dense)

    @pl.loop(1, R)
    def _(k):
        pl.semaphore_signal(barrier, inc=1, device_id={"rows": up(k)})

    @pl.loop(1, G)
    def _(k):
        pl.semaphore_signal(barrier, inc=1, device_id={"grp": gup(k)})

    tab_copy = pltpu.make_async_copy(tab_hbm, tab, local_sem.at[0])
    w_copy = pltpu.make_async_copy(w_hbm, w, local_sem.at[1])
    tab_copy.start()
    w_copy.start()

    clear = sent_short if paired else total - 16
    rows[:, clear:total] = jnp.zeros((R, total - clear, emb), BF16)
    g_recv[:, total - 16 : total] = jnp.zeros((R, 16, emb), BF16)
    idx_ref[...] = jnp.zeros_like(idx_ref)
    idx_ref[2:3, 0:bdev] = lab_ref[...]
    for t in range(3):
        for f in range(fgrp):
            lanes = pl.ds(t * per + f * bdev, bdev)
            owner = own_ref[f, t : t + 1, :]
            idx_ref[0:1, lanes] = owner * 8 + t
            idx_ref[1:2, lanes] = off_ref[f, t : t + 1, :]
            idx_ref[3:4, lanes] = owner * width + (t * (cap // 3) - starts[t])
    for j in range(nl // 128):
        col[pl.ds(j * 128, 128), :] = idx_ref[:, pl.ds(j * 128, 128)].T
    for t in range(3):
        at = pl.ds(t * per, per)
        of[at, :] = ones_where(iota((per, n_rows), 1) == col[at, 1:2])
    owner_hot = ones_where(iota((r8, nl), 0) == idx_ref[0:1, :])
    present = mm(owner_hot, of[...]) > 0.5
    before = ones_where(iota((n_rows, n_rows), 0) < iota((n_rows, n_rows), 1))
    ranked = jnp.where(present, mm(ones_where(present), before), -1.0)
    ranked_bf[...] = ranked.astype(BF16)
    req_send[...] = ranked.reshape(R, 8, n_rows)[:, 0:4].astype(BF16)

    tab_copy.wait()
    tb[...] = tab[...].astype(BF16)
    pl.semaphore_wait(barrier, R - 1 + G - 1)

    def req_copy(k):
        return pltpu.make_async_remote_copy(
            req_send.at[up(k)], req_recv.at[me], ss0.at[k], rs0.at[me],
            device_id={"rows": up(k)}, device_id_type=pl.DeviceIdType.MESH,
        )

    def req_arrival(src):
        return pltpu.make_async_remote_copy(
            req_send.at[src], req_recv.at[src], ss0.at[0], rs0.at[src],
            device_id={"rows": src}, device_id_type=pl.DeviceIdType.MESH,
        )

    @pl.loop(1, R)
    def _(k):
        req_copy(k).start()

    if paired:
        @pl.when(inner == 1)
        def _():
            dense_copy(0).start()

    req_recv[me] = req_send[me]

    def fetch(src):
        @pl.when(src != me)
        def _():
            req_arrival(src).wait_recv()

        rank = req_recv[src].astype(F32)
        bands = []
        for t in range(3):
            shift = t * (cap // 3) - starts[t]
            line = (iota((width, n_rows), 0) - shift).astype(F32)
            line = jnp.where(line < 0.0, -2.0, line)
            bands.append(mm(ones_where(line == rank[t : t + 1, :]), tb[t]))
        fet_send[src] = joined(bands)

    rows_start, rows_wait, rows_drain = exchange(fetch, fet_send, rows, ss1, rs1, paired)
    rows_start()
    if paired:
        @pl.when(inner == 1)
        def _():
            dense_wait(side_of)
            for j in range(1, 3):
                dense_copy(j).start()

    for t in range(3):
        at = pl.ds(t * per, per)
        own_hot = ones_where(iota((per, r8), 1) == col[at, 0:1])
        picked = mm(own_hot, ranked_bf[...]) * of[at, :].astype(F32)
        slot = jnp.sum(picked, axis=1, keepdims=True) + col[at, 3:4].astype(F32)
        looked[t] = jnp.broadcast_to(slot, (per, emb))

    lane_slot = iota((per, chunk), 1).astype(F32)
    slot_rows = []
    for t in range(3):
        slot = looked[t]
        for c in range(CHUNKS):
            p_ref[t, c] = ones_where(lane_slot == slot[:, 0:1] - float(c * chunk))
        slot_rows.append(slot.T[0:1, :])
    for t in range(3):
        pt_ref[t] = ones_where(iota((slots, per), 0).astype(F32) == slot_rows[t])
    req_cols = req_recv[...].astype(F32).reshape(R * 4, n_rows).T.astype(BF16)
    row_i = iota((R * 4, chunk), 0)
    slot_in = iota((n_rows, chunk), 1) & (width - 1)
    for t in range(3):
        line = (slot_in - (t * (cap // 3) - starts[t])).astype(F32)
        line = jnp.where(line < 0.0, -2.0, line)
        for c in range(CHUNKS):
            col_j = iota((R * 4, chunk), 1) + c * chunk
            first = (row_i >> 2) * width
            spread = ones_where(((row_i & 3) == t) & (col_j >= first) & (col_j < first + width))
            st_ref[t, c] = ones_where(mm(req_cols, spread) == line)

    w_copy.wait()
    for f in range(fgrp):
        w_t[:, f * emb : (f + 1) * emb] = w[f * emb : (f + 1) * emb, :].T

    def arrived(ref, n, t):
        src = pl.ds(nth_chunk(n) * fan, fan)
        return ref[src, starts[t] : starts[t] + width].reshape(chunk, emb)

    for n in range(CHUNKS):
        rows_wait(n)
        for t in range(3):
            part = mm(p_ref[t, nth_chunk(n)], arrived(rows, n, t))
            looked[t] = part if n == 0 else looked[t] + part
        if paired and n == DENSE_AT:
            at = pl.ds(2 * per, per)
            keys = []
            for ys in range(2):
                used = served(far_inner, ys, my_chunk, side_of)

                @pl.when(used * (1 - inner * same(side_of, ys)) == 1)
                def _():
                    dense_wait(ys)

                key = ((far_inner * fan + ys) * 8 + 2) * used - (1 - used)
                keys.append(key)
                part = jnp.where(col[at, 0:1] == key, mm(of[at, :], dense[ys]), 0.0)
                dense_part[...] = part if ys == 0 else dense_part[...] + part
    if paired:
        hit = (col[at, 0:1] == keys[0]) | (col[at, 0:1] == keys[1])
        looked[2] = jnp.where(hit, dense_part[...], looked[2])
    embedded = (looked[0] * looked[1] + looked[2]).astype(BF16)
    features = jnp.concatenate(
        [embedded[f * bdev : (f + 1) * bdev] for f in range(fgrp)], axis=1
    )
    hidden = w.shape[1]
    half = G // 2
    side = lax.rem(mg, 2)
    partner = mg + 1 - 2 * side
    mine = lax.div(mg, 2)

    def swap(c):
        return pltpu.make_async_remote_copy(
            part_send.at[c, 1 - side], swap_recv.at[c], ssp.at[c], rsp.at[c],
            device_id={"grp": partner}, device_id_type=pl.DeviceIdType.MESH,
        )

    def part_copy(k, c):
        return pltpu.make_async_remote_copy(
            pair_send.at[c], pair_recv.at[k, c], ssp.at[k * PARTS + c], rsp.at[k * PARTS + c],
            device_id={"grp": lax.rem(mg + 2 * k, G)}, device_id_type=pl.DeviceIdType.MESH,
        )

    def gp_copy(c):
        return pltpu.make_async_remote_copy(
            gp.at[c, side], gp.at[c, side], ssg.at[c], rsg.at[c],
            device_id={"grp": partner}, device_id_type=pl.DeviceIdType.MESH,
        )

    piece = hidden // PARTS
    for c in range(PARTS):
        partial = mm(features, w[:, c * piece : (c + 1) * piece])
        for g in range(G):
            block = partial[g * share : (g + 1) * share]
            part_f32[c, g % 2, g // 2] = block
            part_send[c, g % 2, g // 2] = block.astype(BF16)
        swap(c).start()
    for c in range(PARTS):
        swap(c).wait_recv()
        pair = part_f32[c, side] + swap_recv[c].astype(F32)
        pair_send[c] = pair.astype(BF16)
        for k in range(1, half):
            part_copy(k, c).start()
        part_f32[c, side] = pair + b_ref[:, c * piece : (c + 1) * piece]
    logits = jnp.zeros((half * share, 1), F32)
    slopes = []
    for c in range(PARTS):
        pre = part_f32[c, side]
        for k in range(1, half):
            part_copy(k, c).wait_recv()
            pre = pre + pair_recv[k, c].astype(F32)
        pre = pre.reshape(half * share, piece)
        sig = jax.nn.sigmoid(pre)
        w_out = wo_ref[:, c * piece : (c + 1) * piece]
        logits = logits + jnp.sum(pre * sig * w_out, axis=1, keepdims=True)
        slopes.append(w_out * (sig * (1.0 + pre * (1.0 - sig))))
    targets = jnp.concatenate(
        [
            col[pl.ds(pl.multiple_of((2 * j + side) * share, share), share), 2:3]
            for j in range(half)
        ],
        axis=0,
    ).astype(F32)
    grad_logit = jax.nn.sigmoid(logits) - targets
    for c in range(PARTS):
        gp[c, side] = (grad_logit * slopes[c]).astype(BF16).reshape(half, share, piece)
        gp_copy(c).start()
    losses = (
        jnp.maximum(logits, 0.0) + jnp.log1p(jnp.exp(-jnp.abs(logits))) - targets * logits
    )
    diag = iota((half * share, share), 0) - mine * share == iota((half * share, share), 1)
    loss_ref[...] = jnp.sum(jnp.where(diag, losses, 0.0), axis=0, keepdims=True)

    grad_emb = None
    for c in range(PARTS):
        gp_copy(c).wait_recv()
        grad_pre = jnp.concatenate([gp[c, g % 2, g // 2] for g in range(G)], axis=0)
        term = mm(grad_pre, w_t[c * piece : (c + 1) * piece, :])
        grad_emb = term if grad_emb is None else grad_emb + term
    for f in range(fgrp):
        at = pl.ds(f * bdev, bdev)
        grad_rows = grad_emb[:, f * emb : (f + 1) * emb]
        rg[0, at, :] = (grad_rows * looked[1, at, :]).astype(BF16)
        rg[1, at, :] = (grad_rows * looked[0, at, :]).astype(BF16)
        rg[2, at, :] = grad_rows.astype(BF16)

    def collect(dst):
        at = pl.ds(pl.multiple_of(dst * width, width), width)
        g_send[dst] = joined([mm(pt_ref[t, at, :], rg[t]) for t in range(3)])

    g_start, g_wait, g_drain = exchange(collect, g_send, g_recv, ss2, rs2, False)
    g_start()

    @pl.loop(1, R)
    def _(k):
        req_copy(k).wait_send()

    rows_drain()
    if paired:
        @pl.when(inner == 1)
        def _():
            for j in range(3):
                dense_copy(j).wait_send()

    for c in range(PARTS):
        swap(c).wait_send()
        gp_copy(c).wait_send()
        for k in range(1, half):
            part_copy(k, c).wait_send()

    for n in range(CHUNKS):
        g_wait(n)
        for t in range(3):
            part = mm(st_ref[t, nth_chunk(n)], arrived(g_recv, n, t))
            tg_ref[t] = part if n == 0 else tg_ref[t] + part

    g_drain()


def store(tg_ref, loss_ref, tg_out, loss_out, sem):
    copies = (
        pltpu.make_async_copy(tg_ref, tg_out, sem.at[0]),
        pltpu.make_async_copy(loss_ref, loss_out, sem.at[1]),
    )
    for copy in copies:
        copy.start()
    for copy in copies:
        copy.wait()


def body(owner, offset, tables, w_first, b_first, w_out, labels):
    R, G = lax.axis_size("rows"), lax.axis_size("grp")
    bdev, fgrp = owner.shape[0], owner.shape[1]
    n_rows, emb = tables.shape[1], tables.shape[2]
    hidden = w_first.shape[1]
    per = bdev * fgrp
    nl = 3 * per
    hot_count = 8 * (per * 7 // (16 * R)) + 8
    uniq = hot_count // 3
    cap = 3 * uniq
    total = -(-cap // 16) * 16
    starts = [t * uniq // 16 * 16 for t in range(3)]
    width = 16
    while any(s + width < (t + 1) * uniq for t, s in enumerate(starts)):
        width *= 2
    total = max(total, max(starts) + width)
    share = bdev // G
    half = G // 2
    slots = R * width
    piece = hidden // PARTS

    owner_rows = owner.transpose(1, 2, 0)
    offset_rows = offset.transpose(1, 2, 0)
    vmem = pl.BlockSpec(memory_space=pltpu.VMEM)
    hbm = pl.BlockSpec(memory_space=pl.ANY)
    sems = pltpu.SemaphoreType.DMA
    table_grad, losses = pl.pallas_call(
        functools.partial(kernel, R, G, cap, fgrp, starts, width),
        out_shape=(
            jax.ShapeDtypeStruct((3, n_rows, emb), F32),
            jax.ShapeDtypeStruct((1, share), F32),
        ),
        in_specs=[vmem, vmem, vmem, hbm, hbm, vmem, vmem],
        out_specs=(vmem, vmem),
        scratch_shapes=[
            pltpu.VMEM((8, nl), jnp.int32),
            pltpu.VMEM((3, n_rows, emb), F32),
            pltpu.VMEM((3, n_rows, emb), BF16),
            pltpu.VMEM(w_first.shape, BF16),
            pltpu.VMEM((hidden, fgrp * emb), BF16),
            pltpu.VMEM((nl, 8), jnp.int32),
            pltpu.VMEM((nl, n_rows), BF16),
            pltpu.VMEM((R * 8, n_rows), BF16),
            pltpu.VMEM((R, 4, n_rows), BF16),
            pltpu.VMEM((R, 4, n_rows), BF16),
            pltpu.VMEM((R, total, emb), BF16),
            pltpu.VMEM((R, total, emb), BF16),
            pltpu.VMEM((2, n_rows if R == 2 * CHUNKS else 16, emb), BF16),
            pltpu.VMEM((per if R == 2 * CHUNKS else 8, emb), F32),
            pltpu.VMEM((3, per, emb), F32),
            pltpu.VMEM((3, CHUNKS, per, slots // CHUNKS), BF16),
            pltpu.VMEM((3, slots, per), BF16),
            pltpu.VMEM((3, CHUNKS, n_rows, slots // CHUNKS), BF16),
            pltpu.VMEM((PARTS, 2, half, share, piece), F32),
            pltpu.VMEM((PARTS, 2, half, share, piece), BF16),
            pltpu.VMEM((PARTS, half, share, piece), BF16),
            pltpu.VMEM((PARTS, half, share, piece), BF16),
            pltpu.VMEM((half, PARTS, half, share, piece), BF16),
            pltpu.VMEM((PARTS, 2, half, share, piece), BF16),
            pltpu.VMEM((3, per, emb), BF16),
            pltpu.VMEM((R, total, emb), BF16),
            pltpu.VMEM((R, total, emb), BF16),
            sems((2,)),
            sems((R,)), sems((R,)), sems((R,)), sems((R,)), sems((R,)), sems((R,)),
            sems((4,)), sems((2,)),
            sems((half * PARTS,)), sems((half * PARTS,)), sems((PARTS,)), sems((PARTS,)),
        ],
        compiler_params=pltpu.CompilerParams(
            collective_id=0, has_side_effects=True, vmem_limit_bytes=(44 if slots <= 1024 else 60) * MIB
        ),
        name="embed_step",
    )(
        *(
            pltpu.with_memory_space_constraint(v, pltpu.HBM)
            for v in (
                owner_rows, offset_rows, labels.reshape(1, bdev), tables, w_first,
                b_first.reshape(1, hidden), w_out.reshape(1, hidden),
            )
        )
    )
    table_grad, losses = pl.pallas_call(
        store,
        out_shape=(
            jax.ShapeDtypeStruct((3, n_rows, emb), F32),
            jax.ShapeDtypeStruct((1, share), F32),
        ),
        in_specs=[vmem, vmem],
        out_specs=(hbm, hbm),
        scratch_shapes=[sems((2,))],
        compiler_params=pltpu.CompilerParams(vmem_limit_bytes=MIB),
        name="store",
    )(table_grad, losses)
    return table_grad, losses.reshape(share)


def solution(mesh):
    placed = (
        P("rows", "grp", None),
        P("rows", "grp", None),
        P("grp", "rows", None),
        P("grp", None),
        P(),
        P(),
        P("rows"),
    )
    return jax.shard_map(
        body,
        mesh=mesh,
        in_specs=placed,
        out_specs=(P("grp", "rows", None), P(("rows", "grp"))),
        check_vma=False,
    )
```
